32 devices in a mesh: replica: 2 (over x), fsdp: 16 (over z, y, core).
Axes of the slice: x: 2, y: 2, z: 4, core: 2. Of those that a mesh axis runs over, the one named last changes fastest.
Arguments:
- act: bfloat16 [2, 2, 6144, 2048], P('replica', None, 'fsdp'), may hold values from -6 to 6
- target: bfloat16 [2, 2, 6144, 512], P('replica', None, 'fsdp'), may hold values from -6 to 6
- weights: float32 [2, 2048, 512], P('replica', 'fsdp'), may hold values from -6 to 6
- inner_m: float32 [2, 2048, 512], P('replica', 'fsdp'), may hold values from -0.0006 to 0.0006
- inner_v: float32 [2, 2048, 512], P('replica', 'fsdp'), may hold values from 2e-09 to 2e-08
- outer_delta: float32 [2, 2048, 512], P('replica', 'fsdp'), may hold values from -4 to 4
- anchor: float32 [2048, 512], P('fsdp'), may hold values from -6 to 6
- outer_mom: float32 [2048, 512], P('fsdp'), may hold values from -1.5 to 1.5
Outputs:
- new_weights: float32 [2, 2048, 512], P('replica', 'fsdp')
- new_m: float32 [2, 2048, 512], P('replica', 'fsdp')
- new_v: float32 [2, 2048, 512], P('replica', 'fsdp')
- new_anchor: float32 [2048, 512], P('fsdp')
- new_mom: float32 [2048, 512], P('fsdp')
The draws below stay inside these ranges and needn't reach their ends.
All inputs are finite; a program needn't handle non-finite values.
Results may differ from the reference program's by a relative error of at most 0.0034.
Values may be sent and summed in bfloat16 or wider, within the bound.
A program may use at most 64 MiB of HBM per device.

```python
import math
import jax
import jax.numpy as jnp
from jax import lax

FEAT = 2048
VDIM = 512
MICRO = 2
TOKENS = 6144
REPLICAS = 2
N_REPLICA = 2


def spiked(values, rng, source, target, parts, factor):
    def block_of(axis_at):
        return (jnp.arange(values.shape[axis_at]) // (values.shape[axis_at] // parts)).reshape((-1,) + (1,) * (values.ndim - 1 - axis_at))

    one_side = jax.random.permutation(rng, parts)[block_of(target)]
    other_side = (block_of(target) + parts // 2) % parts
    return jnp.where((block_of(source) == one_side) | (block_of(source) == other_side), factor * values, values)


def block_levels(rng, extent, shards, least, high):
    def one(position, parts):
        steps = jax.random.uniform(jax.random.fold_in(jax.random.fold_in(rng, 6), position), (parts,), jnp.float32, least / len(shards), high / len(shards))
        return jnp.repeat(jnp.exp(steps), extent[position] // parts).reshape((-1,) + (1,) * (len(extent) - position - 1))

    level = one(*shards[0])
    for cut in shards[1:]:
        level = level * one(*cut)
    return level


def scatter_about(stream_key, dims, width, most, pieces=(), held_as=jnp.bfloat16):
    loudness = block_levels(stream_key, dims, pieces, -0.22, 0.18) if pieces else 1.0
    array = jax.random.normal(stream_key, dims, jnp.float32) * width * loudness
    return jnp.minimum(jnp.maximum(array, -most), most).astype(held_as)


def gaussian_with(rng, dims, width, reach, split, heavy, held_as=jnp.bfloat16):
    entries = width * jax.random.normal(rng, dims, jnp.float32)
    if split:
        entries = entries * block_levels(rng, dims, split, -0.22, 0.18)
    return jnp.clip(spiked(entries, jax.random.fold_in(rng, 3), *heavy), -reach, reach).astype(held_as)


def setup_inputs(seed: int = 0) -> dict:
    key_of = jax.random.split(jax.random.key(seed), 9)
    act = gaussian_with(key_of[0], (REPLICAS, MICRO, TOKENS, FEAT), 1.0, 6.0, ((0, 2), (2, 16)), (2, 3, 16, 2.0))
    target = scatter_about(key_of[1], (REPLICAS, MICRO, TOKENS, VDIM), 1.0, 6.0, ((0, 2), (2, 16)))
    weights = scatter_about(key_of[2], (REPLICAS, FEAT, VDIM), 1.0, 6.0, ((0, 2), (1, 16)), jnp.float32)
    inner_m = scatter_about(key_of[3], (REPLICAS, FEAT, VDIM), 0.0001, 0.0006, ((0, 2), (1, 16)), jnp.float32)
    inner_v = jnp.clip(jnp.exp(math.log(1.999999987845058e-08) - 2.3025851 * jax.random.uniform(key_of[4], (REPLICAS, FEAT, VDIM), jnp.float32) ** block_levels(key_of[4], (REPLICAS, FEAT, VDIM), ((0, 2), (1, 16)), -0.2, 0.2)), 1.999999943436137e-09, 1.999999987845058e-08)
    outer_delta = scatter_about(key_of[5], (REPLICAS, FEAT, VDIM), 0.3, 4.0, ((0, 2), (1, 16)), jnp.float32)
    anchor = scatter_about(key_of[6], (FEAT, VDIM), 1.0, 6.0, ((0, 16),), jnp.float32)
    outer_mom = scatter_about(key_of[7], (FEAT, VDIM), 0.1, 1.5, ((0, 16),), jnp.float32)
    return {"act": act, "target": target, "weights": weights, "inner_m": inner_m, "inner_v": inner_v, "outer_delta": outer_delta, "anchor": anchor, "outer_mom": outer_mom}


def reference(act, target, weights, inner_m, inner_v, outer_delta, anchor, outer_mom):
    in_scale = FEAT ** (-0.5)
    mean_delta = lax.optimization_barrier(jnp.sum(outer_delta, axis=0)) / N_REPLICA
    new_mom = 0.9 * outer_mom + mean_delta
    new_anchor = anchor - 0.7 * (mean_delta + 0.9 * new_mom)
    mixed_list = []
    moment_list = []
    second_list = []
    for replica_id in range(N_REPLICA):
        flat_act = act[replica_id].reshape(MICRO * TOKENS, FEAT)
        low = weights[replica_id].astype(jnp.bfloat16)
        predicted = jnp.dot(flat_act, low, preferred_element_type=jnp.float32) * in_scale
        wanted = target[replica_id].reshape(MICRO * TOKENS, VDIM).astype(jnp.float32)
        resid = (predicted - wanted).astype(jnp.bfloat16)
        grad = lax.dot_general(flat_act, resid, (((0,), (0,)), ((), ())), preferred_element_type=jnp.float32)
        grad = grad * (in_scale / (MICRO * TOKENS))
        moment = 0.9 * inner_m[replica_id] + 0.1 * grad
        second = 0.95 * inner_v[replica_id] + 0.05 * grad * grad
        trained = weights[replica_id] - 0.3 * moment / (jnp.sqrt(second) + 1e-08)
        mixed_list.append(0.5 * trained + 0.5 * new_anchor)
        moment_list.append(moment)
        second_list.append(second)
    return (jnp.stack(mixed_list), jnp.stack(moment_list), jnp.stack(second_list), new_anchor, new_mom)
```

```python
import functools

import jax
import jax.numpy as jnp
from jax import lax
from jax.experimental import pallas as pl
from jax.experimental.pallas import tpu as pltpu
from jax.sharding import PartitionSpec as P

MESH = pl.DeviceIdType.MESH
PIECES = 2
LIMIT = 16


def flip(me, mask):
    out = me
    bit = 1
    while bit <= mask:
        if mask & bit:
            out = out + bit * (1 - 2 * ((me // bit) % 2))
        bit *= 2
    return out


def low(k):
    return k & -k


def arrivals(n):
    labels = [k for k in range(2, n, 2)]

    def when(k):
        return (bin(k).count("1"), -low(k)) if low(k) > 2 or k == 2 else (bin(k).count("1") + 1, -k)

    return sorted(labels, key=when)


def kernel(
    n, pieces, in_scale,
    act, target, weights, delta,
    grad_out, peer_out,
    wf, w, a, at, acc, tgt, res, g, sb, rb,
    w_sem, a_sem, t_sem, ag_send, ag_recv, rs_send, rs_recv, d_send, d_recv,
):
    me = lax.axis_index("fsdp")
    rep = lax.axis_index("replica")
    core = me % 2
    rows = weights.shape[0]
    part = rows // pieces
    pairs = n // 2
    width = 2 * rows
    tokens = act.shape[0]
    tile = 256 if tokens % 256 == 0 else tokens

    bits = [1 << j for j in range(n.bit_length() - 1)]

    w_copy = pltpu.make_async_copy(weights, wf, w_sem)
    w_copy.start()
    barrier = pltpu.get_barrier_semaphore()
    for b in bits:
        pl.semaphore_signal(barrier, inc=1, device_id=(rep, flip(me, b)), device_id_type=MESH)
    pl.semaphore_signal(barrier, inc=1, device_id=(1 - rep, me), device_id_type=MESH)
    a_copies = []
    for m in range(pairs):
        col = pl.multiple_of((flip(me, 2 * m) // 2) * width, width)
        a_copies.append(
            pltpu.make_async_copy(act.at[:, pl.ds(col, width)], a.at[m], a_sem.at[m])
        )
        a_copies[-1].start()
    t_copy = pltpu.make_async_copy(target, tgt, t_sem)
    t_copy.start()

    def spot(k, p):
        owner_core = core if k % 2 == 0 else 1 - core
        return pl.ds(pl.multiple_of(owner_core * rows + p * part, part), part)

    w_copy.wait()
    w[0, pl.ds(pl.multiple_of(core * rows, rows), rows), :] = wf[...].astype(jnp.bfloat16)
    pl.semaphore_wait(barrier, len(bits) + 1)

    def ag_copy(k, b, p):
        return pltpu.make_async_remote_copy(
            src_ref=w.at[k // 2, spot(k, p)],
            dst_ref=w.at[(k + b) // 2, spot(k, p)],
            send_sem=ag_send.at[k + b, p],
            recv_sem=ag_recv.at[k + b, p],
            device_id=(rep, flip(me, b)),
            device_id_type=MESH,
        )

    for b in reversed(bits):
        for p in range(pieces):
            ag_copy(0, b, p).start()
    d_copy = pltpu.make_async_remote_copy(
        src_ref=delta, dst_ref=peer_out, send_sem=d_send, recv_sem=d_recv,
        device_id=(1 - rep, me), device_id_type=MESH,
    )
    d_copy.start()

    turned = [False] * pairs

    def turn(m):
        if turned[m]:
            return
        turned[m] = True
        a_copies[m].wait()
        for t in range(0, tokens, tile):
            at[m, :, t : t + tile] = a[m, t : t + tile, :].T

    started = []

    def multiply(m):
        turn(m)
        first = not started
        started.append(m)

        @pl.loop(0, tokens // tile)
        def _(t):
            sl = pl.ds(pl.multiple_of(t * tile, tile), tile)
            prod = jnp.dot(a[m, sl, :], w[m], preferred_element_type=jnp.float32)
            if first:
                acc[sl, :] = prod
            else:
                acc[sl, :] += prod

    def got(k):
        b = low(k)
        for p in range(pieces):
            ag_copy(k - b, b, p).wait_recv()
            for c in reversed(bits):
                if c < b:
                    ag_copy(k, c, p).start()

    def finish(m):
        got(2 * m + 1)
        multiply(m)

    turn(0)
    finish(0)
    order = arrivals(n)
    pending = []
    for m, k in enumerate(order):
        turn(k // 2)
        got(k)
        if pending:
            finish(pending.pop(0))
        pending.append(k // 2)
    for m in pending:
        finish(m)

    t_copy.wait()

    @pl.loop(0, tokens // tile)
    def _(t):
        sl = pl.ds(pl.multiple_of(t * tile, tile), tile)
        res[sl, :] = (acc[sl, :] * in_scale - tgt[sl, :].astype(jnp.float32)).astype(jnp.bfloat16)

    mine = pl.ds(pl.multiple_of(core * rows, rows), rows)
    theirs = pl.ds(pl.multiple_of((1 - core) * rows, rows), rows)

    def rs_copy(k, p):
        b = low(k)
        where = pl.ds(p * part, part)
        if b == 1:
            where = pl.ds(0, rows)
        return pltpu.make_async_remote_copy(
            src_ref=sb.at[k, where],
            dst_ref=rb.at[k, where],
            send_sem=rs_send.at[k, p],
            recv_sem=rs_recv.at[k, p],
            device_id=(rep, flip(me, b)),
            device_id_type=MESH,
        )

    def produce(m):
        g[m] = jnp.dot(at[m], res[...], preferred_element_type=jnp.float32)
        sb[2 * m + 1] = g[m, theirs, :].astype(jnp.bfloat16)
        rs_copy(2 * m + 1, 0).start()

    def collect(k):
        b = low(k) if k else n
        rs_copy(k + 1, 0).wait_recv()
        base = pl.multiple_of(core * rows, rows)
        for p in range(pieces):
            total = g[k // 2, pl.ds(base + p * part, part), :] + rb[k + 1, p * part : (p + 1) * part, :].astype(jnp.float32)
            for c in bits[1:]:
                if c < b:
                    rs_copy(k + c, p).wait_recv()
                    total += rb[k + c, p * part : (p + 1) * part, :].astype(jnp.float32)
            if k:
                sb[k, p * part : (p + 1) * part, :] = total.astype(jnp.bfloat16)
                rs_copy(k, p).start()
            else:
                grad_out[p * part : (p + 1) * part, :] = total

    first = [k for k in range(n - 2, 0, -4)]
    rest = [k for k in range(n - 4, -1, -4)]
    waiting = []
    for k in first:
        produce(k // 2)
        if waiting:
            collect(waiting.pop(0))
        waiting.append(k)
    for k in rest:
        produce(k // 2)
        if waiting:
            collect(waiting.pop(0))
    for k in rest:
        collect(k)

    for k in range(1, n):
        b = low(k)
        for p in range(pieces):
            ag_copy(k - b, b, p).wait_send()
            if b > 1 or p == 0:
                rs_copy(k, p).wait_send()
    d_copy.wait()


def fused(n, act, target, weights, delta):
    tokens, feats = act.shape
    rows, width = weights.shape
    dma = pltpu.SemaphoreType.DMA
    bf, f32 = jnp.bfloat16, jnp.float32
    return pl.pallas_call(
        functools.partial(kernel, n, PIECES, feats ** (-0.5)),
        out_shape=(
            jax.ShapeDtypeStruct((rows, width), f32),
            jax.ShapeDtypeStruct((rows, width), f32),
        ),
        in_specs=[pl.BlockSpec(memory_space=pl.ANY)] * 4,
        out_specs=(pl.BlockSpec(memory_space=pltpu.VMEM), pl.BlockSpec(memory_space=pl.ANY)),
        scratch_shapes=[
            pltpu.VMEM((rows, width), f32),
            pltpu.VMEM((n // 2, 2 * rows, width), bf),
            pltpu.VMEM((n // 2, tokens, 2 * rows), bf),
            pltpu.VMEM((n // 2, 2 * rows, tokens), bf),
            pltpu.VMEM((tokens, width), f32),
            pltpu.VMEM((tokens, width), bf),
            pltpu.VMEM((tokens, width), bf),
            pltpu.VMEM((n // 2, 2 * rows, width), f32),
            pltpu.VMEM((n, rows, width), bf),
            pltpu.VMEM((n, rows, width), bf),
            dma, dma((n // 2,)), dma,
            dma((n, PIECES)), dma((n, PIECES)), dma((n, PIECES)), dma((n, PIECES)),
            dma, dma,
        ],
        compiler_params=pltpu.CompilerParams(collective_id=0, has_side_effects=True),
    )(act, target, weights, delta)


def plain_grad(act, target, low_rows, in_scale):
    whole = lax.all_gather(low_rows, "fsdp", axis=0, tiled=True)
    predicted = jnp.dot(act, whole, preferred_element_type=jnp.float32) * in_scale
    resid = (predicted - target.astype(jnp.float32)).astype(jnp.bfloat16)
    part = lax.dot_general(act, resid, (((0,), (0,)), ((), ())), preferred_element_type=jnp.float32)
    return lax.psum_scatter(part, "fsdp", scatter_dimension=0, tiled=True)


def plain_outer(outer_delta, anchor, outer_mom):
    groups = lax.axis_size("replica")
    block = anchor.shape[1] // groups
    blocks = lax.all_to_all(outer_delta, "replica", split_axis=2, concat_axis=0, tiled=True)
    mean = jnp.sum(blocks, axis=0) / groups
    offset = lax.axis_index("replica") * block
    mom = 0.9 * lax.dynamic_slice_in_dim(outer_mom, offset, block, 1) + mean
    anchor = lax.dynamic_slice_in_dim(anchor, offset, block, 1) - 0.7 * (mean + 0.9 * mom)
    return (
        lax.all_gather(anchor, "replica", axis=1, tiled=True),
        lax.all_gather(mom, "replica", axis=1, tiled=True),
    )


def body(act, target, weights, inner_m, inner_v, outer_delta, anchor, outer_mom):
    n = lax.axis_size("fsdp")
    groups = lax.axis_size("replica")
    micro, tok, feats = act.shape[1:]
    width = weights.shape[2]
    in_scale = feats ** (-0.5)
    flat_act = act[0].reshape(micro * tok, feats)
    flat_target = target[0].reshape(micro * tok, width)
    fits = groups == 2 and 4 <= n <= LIMIT and n & (n - 1) == 0
    if fits:
        grad_rows, peer = fused(n, flat_act, flat_target, weights[0], outer_delta[0])
        mean = (outer_delta[0] + peer) / groups
        new_mom = 0.9 * outer_mom + mean
        new_anchor = anchor - 0.7 * (mean + 0.9 * new_mom)
    else:
        grad_rows = plain_grad(flat_act, flat_target, weights[0].astype(jnp.bfloat16), in_scale)
        new_anchor, new_mom = plain_outer(outer_delta, anchor, outer_mom)
    grad = grad_rows * (in_scale / (micro * tok * n))
    moment = 0.9 * inner_m[0] + 0.1 * grad
    second = 0.95 * inner_v[0] + 0.05 * grad * grad
    trained = weights[0] - 0.3 * moment / (jnp.sqrt(second) + 1e-08)
    mixed = 0.5 * trained + 0.5 * new_anchor
    return (mixed[None], moment[None], second[None], new_anchor, new_mom)


def solution(mesh):
    split = P("replica", None, "fsdp", None)
    both = P("replica", "fsdp", None)
    one = P("fsdp", None)
    return jax.shard_map(
        body,
        mesh=mesh,
        in_specs=(split, split, both, both, both, both, one, one),
        out_specs=(both, both, both, one, one),
        check_vma=False,
    )
```

```python
import functools

import jax
import jax.numpy as jnp
from jax import lax
from jax.experimental import pallas as pl
from jax.experimental.pallas import tpu as pltpu
from jax.sharding import PartitionSpec as P

MESH = pl.DeviceIdType.MESH
PIECES = 2
LIMIT = 16


def flip(me, mask):
    out = me
    bit = 1
    while bit <= mask:
        if mask & bit:
            out = out + bit * (1 - 2 * ((me // bit) % 2))
        bit *= 2
    return out


def low(k):
    return k & -k


def arrivals(n):
    labels = [k for k in range(2, n, 2)]

    def when(k):
        return (bin(k).count("1"), -low(k)) if low(k) > 2 or k == 2 else (bin(k).count("1") + 1, -k)

    return sorted(labels, key=when)


def kernel(
    n, pieces, in_scale,
    act, target, weights, delta,
    grad_out, peer_out,
    wf, w, a, at, acc, tgt, res, g, sb, rb,
    w_sem, a_sem, t_sem, ag_send, ag_recv, rs_send, rs_recv, d_send, d_recv,
):
    me = lax.axis_index("fsdp")
    rep = lax.axis_index("replica")
    core = me % 2
    rows = weights.shape[0]
    part = rows // pieces
    pairs = n // 2
    width = 2 * rows
    tokens = act.shape[0]
    tile = 256 if tokens % 256 == 0 else tokens

    bits = [1 << j for j in range(n.bit_length() - 1)]

    w_copy = pltpu.make_async_copy(weights, wf, w_sem)
    w_copy.start()
    barrier = pltpu.get_barrier_semaphore()
    for b in bits:
        pl.semaphore_signal(barrier, inc=1, device_id=(rep, flip(me, b)), device_id_type=MESH)
    pl.semaphore_signal(barrier, inc=1, device_id=(1 - rep, me), device_id_type=MESH)
    a_copies = []
    for m in range(pairs):
        col = pl.multiple_of((flip(me, 2 * m) // 2) * width, width)
        a_copies.append(
            pltpu.make_async_copy(act.at[:, pl.ds(col, width)], a.at[m], a_sem.at[m])
        )
        a_copies[-1].start()
    t_copy = pltpu.make_async_copy(target, tgt, t_sem)
    t_copy.start()

    def spot(k, p):
        owner_core = core if k % 2 == 0 else 1 - core
        return pl.ds(pl.multiple_of(owner_core * rows + p * part, part), part)

    w_copy.wait()
    w[0, pl.ds(pl.multiple_of(core * rows, rows), rows), :] = wf[...].astype(jnp.bfloat16)
    pl.semaphore_wait(barrier, len(bits) + 1)

    def ag_copy(k, b, p):
        return pltpu.make_async_remote_copy(
            src_ref=w.at[k // 2, spot(k, p)],
            dst_ref=w.at[(k + b) // 2, spot(k, p)],
            send_sem=ag_send.at[k + b, p],
            recv_sem=ag_recv.at[k + b, p],
            device_id=(rep, flip(me, b)),
            device_id_type=MESH,
        )

    for p in range(pieces):
        for b in reversed(bits):
            ag_copy(0, b, p).start()
    d_copy = pltpu.make_async_remote_copy(
        src_ref=delta, dst_ref=peer_out, send_sem=d_send, recv_sem=d_recv,
        device_id=(1 - rep, me), device_id_type=MESH,
    )
    d_copy.start()

    turned = [False] * pairs

    def turn(m):
        if turned[m]:
            return
        turned[m] = True
        a_copies[m].wait()
        for t in range(0, tokens, tile):
            at[m, :, t : t + tile] = a[m, t : t + tile, :].T

    started = []

    def multiply(m):
        turn(m)
        first = not started
        started.append(m)

        @pl.loop(0, tokens // tile)
        def _(t):
            sl = pl.ds(pl.multiple_of(t * tile, tile), tile)
            prod = jnp.dot(a[m, sl, :], w[m], preferred_element_type=jnp.float32)
            if first:
                acc[sl, :] = prod
            else:
                acc[sl, :] += prod

    def got(k):
        b = low(k)
        for p in range(pieces):
            ag_copy(k - b, b, p).wait_recv()
            for c in reversed(bits):
                if c < b:
                    ag_copy(k, c, p).start()

    def finish(m):
        got(2 * m + 1)
        multiply(m)

    turn(0)
    finish(0)
    order = arrivals(n)
    pending = []
    for m, k in enumerate(order):
        turn(k // 2)
        got(k)
        if pending:
            finish(pending.pop(0))
        pending.append(k // 2)
    for m in pending:
        finish(m)

    t_copy.wait()

    @pl.loop(0, tokens // tile)
    def _(t):
        sl = pl.ds(pl.multiple_of(t * tile, tile), tile)
        res[sl, :] = (acc[sl, :] * in_scale - tgt[sl, :].astype(jnp.float32)).astype(jnp.bfloat16)

    mine = pl.ds(pl.multiple_of(core * rows, rows), rows)
    theirs = pl.ds(pl.multiple_of((1 - core) * rows, rows), rows)

    def rs_copy(k, p):
        b = low(k)
        where = pl.ds(p * part, part)
        if b == 1:
            where = pl.ds(0, rows)
        return pltpu.make_async_remote_copy(
            src_ref=sb.at[k, where],
            dst_ref=rb.at[k, where],
            send_sem=rs_send.at[k, p],
            recv_sem=rs_recv.at[k, p],
            device_id=(rep, flip(me, b)),
            device_id_type=MESH,
        )

    def produce(m):
        g[m] = jnp.dot(at[m], res[...], preferred_element_type=jnp.float32)
        sb[2 * m + 1] = g[m, theirs, :].astype(jnp.bfloat16)
        rs_copy(2 * m + 1, 0).start()

    def collect(k):
        b = low(k) if k else n
        rs_copy(k + 1, 0).wait_recv()
        base = pl.multiple_of(core * rows, rows)
        for p in range(pieces):
            total = g[k // 2, pl.ds(base + p * part, part), :] + rb[k + 1, p * part : (p + 1) * part, :].astype(jnp.float32)
            for c in bits[1:]:
                if c < b:
                    rs_copy(k + c, p).wait_recv()
                    total += rb[k + c, p * part : (p + 1) * part, :].astype(jnp.float32)
            if k:
                sb[k, p * part : (p + 1) * part, :] = total.astype(jnp.bfloat16)
                rs_copy(k, p).start()
            else:
                grad_out[p * part : (p + 1) * part, :] = total

    first = [k for k in range(n - 2, 0, -4)]
    rest = [k for k in range(n - 4, -1, -4)]
    waiting = []
    for k in first:
        produce(k // 2)
        if waiting:
            collect(waiting.pop(0))
        waiting.append(k)
    for k in rest:
        produce(k // 2)
        if waiting:
            collect(waiting.pop(0))
    for k in rest:
        collect(k)

    for k in range(1, n):
        b = low(k)
        for p in range(pieces):
            ag_copy(k - b, b, p).wait_send()
            if b > 1 or p == 0:
                rs_copy(k, p).wait_send()
    d_copy.wait()


def fused(n, act, target, weights, delta):
    tokens, feats = act.shape
    rows, width = weights.shape
    dma = pltpu.SemaphoreType.DMA
    bf, f32 = jnp.bfloat16, jnp.float32
    return pl.pallas_call(
        functools.partial(kernel, n, PIECES, feats ** (-0.5)),
        out_shape=(
            pltpu.VMEM((rows, width), f32),
            pltpu.VMEM((rows, width), f32),
        ),
        in_specs=[pl.BlockSpec(memory_space=pl.ANY)] * 4,
        out_specs=(pl.BlockSpec(memory_space=pltpu.VMEM), pl.BlockSpec(memory_space=pltpu.VMEM)),
        scratch_shapes=[
            pltpu.VMEM((rows, width), f32),
            pltpu.VMEM((n // 2, 2 * rows, width), bf),
            pltpu.VMEM((n // 2, tokens, 2 * rows), bf),
            pltpu.VMEM((n // 2, 2 * rows, tokens), bf),
            pltpu.VMEM((tokens, width), f32),
            pltpu.VMEM((tokens, width), bf),
            pltpu.VMEM((tokens, width), bf),
            pltpu.VMEM((n // 2, 2 * rows, width), f32),
            pltpu.VMEM((n, rows, width), bf),
            pltpu.VMEM((n, rows, width), bf),
            dma, dma((n // 2,)), dma,
            dma((n, PIECES)), dma((n, PIECES)), dma((n, PIECES)), dma((n, PIECES)),
            dma, dma,
        ],
        compiler_params=pltpu.CompilerParams(collective_id=0, has_side_effects=True),
    )(act, target, weights, delta)


def plain_grad(act, target, low_rows, in_scale):
    whole = lax.all_gather(low_rows, "fsdp", axis=0, tiled=True)
    predicted = jnp.dot(act, whole, preferred_element_type=jnp.float32) * in_scale
    resid = (predicted - target.astype(jnp.float32)).astype(jnp.bfloat16)
    part = lax.dot_general(act, resid, (((0,), (0,)), ((), ())), preferred_element_type=jnp.float32)
    return lax.psum_scatter(part, "fsdp", scatter_dimension=0, tiled=True)


def plain_outer(outer_delta, anchor, outer_mom):
    groups = lax.axis_size("replica")
    block = anchor.shape[1] // groups
    blocks = lax.all_to_all(outer_delta, "replica", split_axis=2, concat_axis=0, tiled=True)
    mean = jnp.sum(blocks, axis=0) / groups
    offset = lax.axis_index("replica") * block
    mom = 0.9 * lax.dynamic_slice_in_dim(outer_mom, offset, block, 1) + mean
    anchor = lax.dynamic_slice_in_dim(anchor, offset, block, 1) - 0.7 * (mean + 0.9 * mom)
    return (
        lax.all_gather(anchor, "replica", axis=1, tiled=True),
        lax.all_gather(mom, "replica", axis=1, tiled=True),
    )


def body(act, target, weights, inner_m, inner_v, outer_delta, anchor, outer_mom):
    n = lax.axis_size("fsdp")
    groups = lax.axis_size("replica")
    micro, tok, feats = act.shape[1:]
    width = weights.shape[2]
    in_scale = feats ** (-0.5)
    flat_act = act[0].reshape(micro * tok, feats)
    flat_target = target[0].reshape(micro * tok, width)
    fits = groups == 2 and 4 <= n <= LIMIT and n & (n - 1) == 0
    if fits:
        grad_rows, peer = fused(n, flat_act, flat_target, weights[0], outer_delta[0])
        mean = (outer_delta[0] + peer) / groups
        new_mom = 0.9 * outer_mom + mean
        new_anchor = anchor - 0.7 * (mean + 0.9 * new_mom)
    else:
        grad_rows = plain_grad(flat_act, flat_target, weights[0].astype(jnp.bfloat16), in_scale)
        new_anchor, new_mom = plain_outer(outer_delta, anchor, outer_mom)
    grad = grad_rows * (in_scale / (micro * tok * n))
    moment = 0.9 * inner_m[0] + 0.1 * grad
    second = 0.95 * inner_v[0] + 0.05 * grad * grad
    trained = weights[0] - 0.3 * moment / (jnp.sqrt(second) + 1e-08)
    mixed = 0.5 * trained + 0.5 * new_anchor
    return (mixed[None], moment[None], second[None], new_anchor, new_mom)


def solution(mesh):
    split = P("replica", None, "fsdp", None)
    both = P("replica", "fsdp", None)
    one = P("fsdp", None)
    return jax.shard_map(
        body,
        mesh=mesh,
        in_specs=(split, split, both, both, both, both, one, one),
        out_specs=(both, both, both, one, one),
        check_vma=False,
    )
```
